32 devices in a mesh: groups: 2 (over x), holders: 16 (over z, y, core).
Axes of the slice: x: 2, y: 2, z: 4, core: 2. Of those that a mesh axis runs over, the one named last changes fastest.
Arguments:
- q_nope: bfloat16 [2, 256, 128], P(None, ('groups', 'holders')), parts along dimension 1, may hold values from -6 to 6
- q_rope: bfloat16 [2, 256, 64], P(None, ('groups', 'holders')), parts along dimension 1, may hold values from -30 to 30
- w_uk: bfloat16 [2, 16, 128, 512], replicated, may hold values from -0.5 to 0.5
- w_uv: bfloat16 [2, 16, 512, 128], replicated, may hold values from -0.25 to 0.25
- new_latent: bfloat16 [2, 16, 576], P(None, 'groups'), parts along dimension 1, may hold values from -33 to 33
- shallow_cache: bfloat16 [1, 256, 512, 576], P(None, ('groups', 'holders')), parts along dimension 1, may hold values from -30 to 30
- slot_positions: int32 [1, 256, 512], P(None, ('groups', 'holders')), parts along dimension 1, may hold values from 0 to 131071
- slab_map: int32 [1, 256], P(None, 'groups'), parts along dimension 1, may hold values from 0 to 127, each once within a row
- deep_cache: bfloat16 [1, 16, 256, 576], P(None, 'groups'), parts along dimension 1, may hold values from -30 to 30
- deep_positions: int32 [1, 16, 256], P(None, 'groups'), parts along dimension 1, may hold values from 0 to 131071
- lengths: int32 [16], P('groups'), parts along dimension 0, may hold values from 1 to 131072
Outputs:
- attended: bfloat16 [2, 256, 128], P(None, ('groups', 'holders')), parts along dimension 1
The draws below stay inside these ranges and needn't reach their ends.
There are 2 independent parts, one for each index of `groups`. The reference program is written for one: setup_inputs(seed, part) draws one part's arguments, and reference() takes and returns one part's arrays. A program takes and returns all parts, laid end to end along the dimension named above; an argument that names none is the same for every part. Nothing has to cross between parts.
Inputs may be any that keep to these rules, and one draw needn't show every extreme that they name: Each row of slab_map names every slot once; entry b * 16 + s is the slot of request b's slab s.
All inputs are finite; a program needn't handle non-finite values.
Results may differ from the reference program's by a relative error of at most 0.0065.
Values may be sent and summed in bfloat16 or wider, within the bound.
A program may use at most 64 MiB of HBM per device.

```python
import jax
import jax.numpy as jnp
from jax import lax

HEADS = 16
LATENT = 512
ROPE_DIM = 64
NOPE_DIM = 128
VALUE_DIM = 128
BATCH = 8
SLAB = 512
DEEP_TOK = 256
CONTEXT = 131072
SHALLOW = 1
DEEP = 1
LAYERS = 2
SLABS_REQ = 16
SLOTS = 128
ROWS = 128


def direction_table(key):
    raw = jax.random.normal(jax.random.fold_in(key, 9001), (LAYERS, ROPE_DIM), jnp.float32)
    return 2.0 * jnp.clip(raw, -3.0, 3.0)


def base_values(key, shape):
    return jnp.clip(jax.random.normal(key, shape, jnp.float32), -6.0, 6.0)


def aligned_keys(key, seed_offset, shape, first_layer):
    direction = direction_table(key)[first_layer:first_layer + shape[0]]
    drawn = base_values(jax.random.fold_in(key, seed_offset), shape)
    token_shape = shape[:3] + (1,)
    chosen = jax.random.bernoulli(jax.random.fold_in(key, seed_offset + 1), 0.125, token_shape)
    level = jax.random.uniform(jax.random.fold_in(key, seed_offset + 2), token_shape, jnp.float32, 0.5, 4.0)
    extra = jnp.where(chosen, level, 0.0) * direction[:, None, None, :]
    rotary = drawn[..., LATENT:] + extra
    return jnp.concatenate([drawn[..., :LATENT], rotary], axis=-1).astype(jnp.bfloat16)


def draw_q_rope(key, part):
    direction = direction_table(key)
    drawn = base_values(jax.random.fold_in(key, 11), (LAYERS, ROWS, ROPE_DIM))
    picked = jax.random.uniform(jax.random.fold_in(key, 12), (LAYERS, ROWS, 1), jnp.float32)
    strength = 4.0 * picked
    return (drawn + strength * direction[:, None, :]).astype(jnp.bfloat16)


def draw_new_latent(key, part):
    direction = direction_table(key)
    drawn = base_values(jax.random.fold_in(key, 41), (LAYERS, BATCH, LATENT + ROPE_DIM))
    level = jax.random.uniform(jax.random.fold_in(key, 42), (LAYERS, BATCH, 1), jnp.float32, 0.0, 4.5)
    rotary = drawn[..., LATENT:] + level * direction[:, None, :]
    return jnp.concatenate([drawn[..., :LATENT], rotary], axis=-1).astype(jnp.bfloat16)


def draw_shallow_cache(key, part):
    return aligned_keys(key, 21, (SHALLOW, SLOTS, SLAB, LATENT + ROPE_DIM), 0)


def draw_deep_cache(key, part):
    return aligned_keys(key, 31, (DEEP, BATCH, DEEP_TOK, LATENT + ROPE_DIM), SHALLOW)


def place_ends(drawn, own_key, low, high):
    shape = drawn.shape
    index_at = [jax.random.randint(jax.random.fold_in(own_key, axis), (), 0, shape[axis]) for axis in range(len(shape))]
    drawn = drawn.at[tuple(index_at)].set(low)
    longest = shape.index(max(shape))
    index_at[longest] = (index_at[longest] + 1) % shape[longest]
    return drawn.at[tuple(index_at)].set(high)


def steps_of(own_key, dims, cuts, smallest, top_value):
    def one(dim, blocks):
        heights = jax.random.uniform(jax.random.fold_in(jax.random.fold_in(own_key, 6), dim), (blocks,), jnp.float32, smallest / len(cuts), top_value / len(cuts))
        return jnp.repeat(jnp.exp(heights), dims[dim] // blocks).reshape((-1,) + (1,) * (len(dims) - dim - 1))

    level = one(*cuts[0])
    for cut in cuts[1:]:
        level = level * one(*cut)
    return level


def centred(key, shape, scale, bound, pieces=(), held_as=jnp.bfloat16):
    values = scale * jax.random.normal(key, shape, jnp.float32)
    if pieces:
        values = values * steps_of(key, shape, pieces, -0.22, 0.18)
    return jnp.clip(values, -bound, bound).astype(held_as)


def setup_inputs(seed: int = 0, part: int = 0) -> dict:
    seeds = jax.random.split(jax.random.key(seed), 12)
    part_keys = jax.random.split(jax.random.fold_in(seeds[11], part), 12)
    return {
        "q_nope": centred(part_keys[0], (LAYERS, ROWS, NOPE_DIM), 1.0, 6.0, ((1, 16),)),
        "q_rope": draw_q_rope(jax.random.fold_in(jax.random.fold_in(seeds[11], part), 71), part),
        "w_uk": centred(seeds[2], (LAYERS, HEADS, NOPE_DIM, LATENT), NOPE_DIM ** -0.5, 0.5),
        "w_uv": centred(seeds[3], (LAYERS, HEADS, LATENT, VALUE_DIM), LATENT ** -0.5, 0.25),
        "new_latent": draw_new_latent(jax.random.fold_in(jax.random.fold_in(seeds[11], part), 71), part),
        "shallow_cache": draw_shallow_cache(jax.random.fold_in(jax.random.fold_in(seeds[11], part), 71), part),
        "slot_positions": place_ends(jax.random.randint(part_keys[6], (SHALLOW, SLOTS, SLAB), 0, CONTEXT), jax.random.fold_in(part_keys[6], 1), 0, CONTEXT - 1).astype(jnp.int32),
        "slab_map": jax.vmap(lambda own: jax.random.permutation(own, SLOTS))(jax.random.split(part_keys[7], SHALLOW)).reshape((SHALLOW, SLOTS)).astype(jnp.int32),
        "deep_cache": draw_deep_cache(jax.random.fold_in(jax.random.fold_in(seeds[11], part), 71), part),
        "deep_positions": place_ends(jax.random.randint(part_keys[9], (DEEP, BATCH, DEEP_TOK), 0, CONTEXT), jax.random.fold_in(part_keys[9], 1), 0, CONTEXT - 1).astype(jnp.int32),
        "lengths": place_ends(jax.random.randint(part_keys[10], (BATCH,), 1, CONTEXT + 1), jax.random.fold_in(part_keys[10], 1), 1, CONTEXT).astype(jnp.int32),
    }


score_scale = 192.0 ** -0.5
neg_fill = -1.0e30


def one_request(items):
    query, keys, positions, length, newlat = items
    qf = query.astype(jnp.float32)
    kf = keys.astype(jnp.float32)
    score = jnp.einsum('hc,ksc->hks', qf, kf, precision=lax.Precision.HIGHEST) * score_scale
    live = (positions < length)[None]
    block_max = jnp.max(jnp.where(live, score, neg_fill), axis=-1)
    weight = jnp.where(live, jnp.exp(jnp.where(live, score - block_max[..., None], 0.0)), 0.0).astype(jnp.bfloat16)
    wf = weight.astype(jnp.float32)
    block_sum = jnp.sum(wf, axis=-1)
    block_out = jnp.einsum('hks,ksc->hkc', wf, kf[..., :LATENT], precision=lax.Precision.HIGHEST)
    newf = newlat.astype(jnp.float32)
    own_score = jnp.sum(qf * newf[None, :], axis=-1) * score_scale
    top = jnp.maximum(own_score, jnp.max(block_max, axis=-1))
    factor = jnp.exp(block_max - top[:, None])
    own_factor = jnp.exp(own_score - top)
    total = own_factor + jnp.sum(block_sum * factor, axis=-1)
    mixed = own_factor[:, None] * newf[None, :LATENT] + jnp.einsum('hk,hkc->hc', factor, block_out, precision=lax.Precision.HIGHEST)
    return (mixed / total[:, None]).astype(jnp.bfloat16)


def reference(q_nope, q_rope, w_uk, w_uv, new_latent, shallow_cache, slot_positions, slab_map, deep_cache, deep_positions, lengths):
    results = []
    for layer in range(LAYERS):
        nope = q_nope[layer].reshape(BATCH, HEADS, NOPE_DIM).astype(jnp.float32)
        q_lat = jnp.einsum('bhd,hdc->bhc', nope, w_uk[layer].astype(jnp.float32), precision=lax.Precision.HIGHEST).astype(jnp.bfloat16)
        query = jnp.concatenate([q_lat, q_rope[layer].reshape(BATCH, HEADS, ROPE_DIM)], axis=-1)
        if layer < SHALLOW:
            order = slab_map[layer]
            keys = shallow_cache[layer][order].reshape(BATCH, SLABS_REQ, SLAB, LATENT + ROPE_DIM)
            positions = slot_positions[layer][order].reshape(BATCH, SLABS_REQ, SLAB)
        else:
            keys = deep_cache[layer - SHALLOW][:, None]
            positions = deep_positions[layer - SHALLOW][:, None]
        mixed = lax.map(one_request, (query, keys, positions, lengths, new_latent[layer]))
        attended = jnp.einsum('bhc,hcv->bhv', mixed.astype(jnp.float32), w_uv[layer].astype(jnp.float32), precision=lax.Precision.HIGHEST)
        results.append(attended.astype(jnp.bfloat16).reshape(ROWS, VALUE_DIM))
    return jnp.stack(results, axis=0)
```

```python
import functools

import jax
import jax.numpy as jnp
from jax import lax
from jax.experimental import pallas as pl
from jax.experimental.pallas import tpu as pltpu
from jax.sharding import PartitionSpec as P

HEADS = 16
LATENT = 512
SLABS_REQ = 16

score_scale = 192.0 ** (-0.5)
neg_fill = -1e30

f32 = jnp.float32
bf16 = jnp.bfloat16


def dot(a, b):
    return lax.dot_general(a, b, (((1,), (0,)), ((), ())), preferred_element_type=f32)


def dot_t(a, b):
    return lax.dot_general(a, b, (((1,), (1,)), ((), ())), preferred_element_type=f32)


def iota(shape, dim):
    return lax.broadcasted_iota(jnp.int32, shape, dim)


def lane_sum(mask, values):
    return jnp.sum(jnp.where(mask, values, jnp.zeros_like(values)), axis=1, keepdims=True)


def row_sum(mask, values):
    return jnp.sum(jnp.where(mask, values, jnp.zeros_like(values)), axis=0, keepdims=True)


def one_hot(mask):
    return jnp.where(mask, 1.0, 0.0).astype(bf16)


def kernel(
    n, dims,
    lengths, q_nope, q_rope, w_uk, w_uv, new_latent, cache, positions, slab_map,
    deep_cache, deep_positions,
    out,
    qn_all, qr_all, qn_deep, qr_deep, uk0, uv0, uk1, uv1, newlat, keys, pos, smap,
    dkeys, dpos, qlat, slot_out, proj, outbox, inbox,
    loc_sem, slab_sem, qn_send, qn_recv, qr_send, qr_recv, o_send, o_recv,
):
    rows_dev, slots, batch = dims
    rows = n * rows_dev
    srows = slots * HEADS
    me = lax.axis_index("holders")
    start = me * rows_dev
    head0 = lax.rem(start, HEADS)
    req = lax.div(start, HEADS)
    pad = max(8, rows_dev)
    unroll = n <= 16

    local = [
        (q_nope.at[0], qn_all.at[me]),
        (q_rope.at[0], qr_all.at[me]),
        (q_nope.at[1], qn_deep),
        (q_rope.at[1], qr_deep),
        (w_uk.at[1, pl.ds(head0, rows_dev)], uk1),
        (new_latent, newlat),
        (deep_positions.at[0], dpos),
        (deep_cache.at[0, req], dkeys),
        (w_uv.at[1, pl.ds(head0, rows_dev)], uv1),
        (slab_map, smap),
        (positions.at[0], pos),
        (w_uk.at[0], uk0),
        (w_uv.at[0], uv0),
    ]
    local = [pltpu.make_async_copy(s, d, loc_sem.at[i]) for i, (s, d) in enumerate(local)]
    slab_copies = [
        pltpu.make_async_copy(cache.at[0, j], keys.at[j], slab_sem.at[j]) for j in range(slots)
    ]

    for c in local[:2]:
        c.start()

    barrier = pltpu.get_barrier_semaphore()

    def greet(k, carry):
        peer = lax.rem(me + k, n)
        pl.semaphore_signal(
            barrier, inc=1, device_id={"holders": peer}, device_id_type=pl.DeviceIdType.MESH
        )
        return carry

    lax.fori_loop(1, n, greet, 0, unroll=unroll)
    for c in local[2:12]:
        c.start()
    for c in slab_copies:
        c.start()
    local[12].start()
    local[0].wait()
    local[1].wait()
    pl.semaphore_wait(barrier, n - 1)

    def remote(src, dst, ssem, rsem, k):
        peer = lax.rem(me + k, n)
        return pltpu.make_async_remote_copy(
            src_ref=src, dst_ref=dst, send_sem=ssem.at[k], recv_sem=rsem.at[k],
            device_id={"holders": peer}, device_id_type=pl.DeviceIdType.MESH,
        )

    def q_copies(k):
        return (
            remote(qn_all.at[me], qn_all.at[me], qn_send, qn_recv, k),
            remote(qr_all.at[me], qr_all.at[me], qr_send, qr_recv, k),
        )

    def send_q(k, carry):
        for c in q_copies(k):
            c.start()
        return carry

    lax.fori_loop(1, n, send_q, 0, unroll=unroll)

    def widen(x):
        if x.shape[0] < pad:
            x = jnp.concatenate([x] * (pad // x.shape[0]), axis=0)
        return x

    own_row = lax.rem(iota((pad, 1), 0), rows_dev)

    def per_head(x, head_of):
        acc = None
        for i in range(rows_dev):
            part = dot(x, head_of(i))
            acc = part if acc is None else jnp.where(own_row == i, part, acc)
        return acc

    for c in local[2:9]:
        c.wait()
    pick = iota((batch, newlat.shape[2]), 0) == req
    new1 = row_sum(pick, newlat[1].astype(f32))
    new0 = row_sum(pick, newlat[0].astype(f32))
    qn1 = widen(qn_deep[...].astype(f32)).astype(bf16)
    qr1 = widen(qr_deep[...].astype(f32)).astype(bf16)
    ql1 = per_head(qn1, lambda i: uk1[i]).astype(bf16)
    score = (dot_t(ql1, dkeys[:, :LATENT]) + dot_t(qr1, dkeys[:, LATENT:])) * score_scale
    where1 = row_sum(iota(dpos.shape, 0) == req, dpos[...])
    live = where1 < lengths[req]
    own_max = jnp.max(jnp.where(live, score, neg_fill), axis=1, keepdims=True)
    weight = jnp.where(live, jnp.exp(jnp.where(live, score - own_max, 0.0)), 0.0).astype(bf16)
    own_sum = jnp.sum(weight.astype(f32), axis=1, keepdims=True)
    own_out = dot(weight, dkeys[:, :LATENT])

    def own_scores(ql, qr, new):
        lat = jnp.sum(ql.astype(f32) * new[:, :LATENT], axis=1, keepdims=True)
        rot = jnp.sum(qr.astype(f32) * new[:, LATENT:], axis=1, keepdims=True)
        return (lat + rot) * score_scale

    own_score = own_scores(ql1, qr1, new1)
    top = jnp.maximum(own_score, own_max)
    own_f = jnp.exp(own_score - top)
    far_f = jnp.exp(own_max - top)
    total = own_f + own_sum * far_f
    mixed = ((own_f * new1[:, :LATENT] + own_out * far_f) / total).astype(bf16)
    attended1 = per_head(mixed, lambda i: uv1[i])
    out[1] = attended1[:rows_dev].astype(bf16)

    for c in local[9:12]:
        c.wait()
    r_s = iota((srows, rows), 0)
    c_s = iota((srows, rows), 1)
    found = smap[...] == me * slots + lax.div(iota((srows, smap.shape[1]), 0), HEADS)
    req_col = lane_sum(found, lax.div(iota((srows, smap.shape[1]), 1), SLABS_REQ))
    len_col = jnp.zeros((srows, 1), jnp.int32)
    for b in range(batch):
        len_col = jnp.where(req_col == b, lengths[b], len_col)
    sel_bh = (lax.div(c_s, HEADS) == req_col) & (lax.rem(c_s, HEADS) == lax.rem(r_s, HEADS))
    sel_hb = (lax.rem(c_s, batch) == req_col) & (lax.div(c_s, batch) == lax.rem(r_s, HEADS))
    sel_bh, sel_hb = one_hot(sel_bh), one_hot(sel_hb)
    r_q = iota((rows, rows), 0)
    c_q = iota((rows, rows), 1)
    perm = (lax.rem(r_q, batch) == lax.div(c_q, HEADS)) & (lax.div(r_q, batch) == lax.rem(c_q, HEADS))
    eye = iota((srows, srows), 0) == iota((srows, srows), 1)
    req_row = row_sum(eye, jnp.broadcast_to(req_col, eye.shape))
    r_t = iota((rows, srows), 0)
    c_t = iota((rows, srows), 1)
    back = (lax.div(r_t, batch) == lax.rem(c_t, HEADS)) & (lax.rem(r_t, batch) == req_row)

    def wait_q(k, carry):
        for c in q_copies(k):
            c.wait_recv()
        return carry

    lax.fori_loop(1, n, wait_q, 0, unroll=unroll)
    qn = qn_all[...].astype(f32).reshape(rows, qn_all.shape[2]).astype(bf16)
    qr = qr_all[...].astype(f32).reshape(rows, qr_all.shape[2]).astype(bf16)
    qn_hb = dot(one_hot(perm), qn)
    for h in range(0, HEADS, 2):
        two = [
            dot(qn_hb[g * batch:(g + 1) * batch].astype(bf16), uk0[g]) for g in (h, h + 1)
        ]
        qlat[h * batch:(h + 2) * batch, :] = jnp.concatenate(two, axis=0).astype(bf16)
    q_slot = dot(sel_hb, qlat[...]).astype(bf16)
    r_slot = dot(sel_bh, qr).astype(bf16)

    maxes, sums = [], []
    for j in range(slots):
        at = slice(j * HEADS, (j + 1) * HEADS)
        slab_copies[j].wait()
        score = (
            dot_t(q_slot[at], keys[j, :, :LATENT]) + dot_t(r_slot[at], keys[j, :, LATENT:])
        ) * score_scale
        live = pos[j:j + 1, :] < len_col[at]
        block_max = jnp.max(jnp.where(live, score, neg_fill), axis=1, keepdims=True)
        weight = jnp.where(
            live, jnp.exp(jnp.where(live, score - block_max, 0.0)), 0.0
        ).astype(bf16)
        maxes.append(block_max)
        sums.append(jnp.sum(weight.astype(f32), axis=1, keepdims=True))
        slot_out[at, :] = dot(weight, keys[j, :, :LATENT])
    slot_max = jnp.concatenate(maxes, axis=0)
    slot_sum = jnp.concatenate(sums, axis=0)

    max_row = row_sum(eye, jnp.broadcast_to(slot_max, eye.shape))
    sum_row = row_sum(eye, jnp.broadcast_to(slot_sum, eye.shape))
    dense_max = jnp.max(jnp.where(back, max_row, neg_fill), axis=1, keepdims=True)
    factor_row = jnp.exp(max_row - row_sum(back, jnp.broadcast_to(dense_max, back.shape)))
    dense_sum = lane_sum(back, jnp.broadcast_to(sum_row * factor_row, back.shape))
    factor_col = lane_sum(eye, jnp.broadcast_to(factor_row, eye.shape))
    scaled = (slot_out[...] * factor_col).astype(bf16)
    dense = dot(one_hot(back), scaled)
    local[12].wait()
    for h in range(HEADS):
        part = dot(dense[h * batch:(h + 1) * batch].astype(bf16), uv0[h])
        proj[pl.ds(h, batch, stride=HEADS), :] = part
    outbox[:, :rows_dev, :] = proj[...].reshape(n, rows_dev, proj.shape[1])
    stat_max = row_sum(perm, jnp.broadcast_to(dense_max, perm.shape))
    stat_sum = row_sum(perm, jnp.broadcast_to(dense_sum, perm.shape))
    stats = jnp.concatenate([stat_max, stat_sum], axis=0)
    outbox[:, rows_dev:, :] = jnp.broadcast_to(stats[None], (n,) + stats.shape)
    inbox[me] = outbox[me]

    def o_copy(k):
        return remote(outbox.at[lax.rem(me + k, n)], inbox.at[me], o_send, o_recv, k)

    def send_o(k, carry):
        o_copy(k).start()
        return carry

    lax.fori_loop(1, n, send_o, 0, unroll=unroll)

    qn0 = widen(qn_all[me].astype(f32)).astype(bf16)
    qr0 = widen(qr_all[me].astype(f32)).astype(bf16)
    ql0 = per_head(qn0, lambda i: uk0[head0 + i]).astype(bf16)
    own_score = own_scores(ql0, qr0, new0)
    new_in = jnp.broadcast_to(new0[:, :LATENT], (pad, LATENT)).astype(bf16)
    new_out = per_head(new_in, lambda i: uv0[head0 + i])

    def wait_sent(k, carry):
        for c in q_copies(k):
            c.wait_send()
        return carry

    lax.fori_loop(1, n, wait_sent, 0, unroll=unroll)

    def wait_o(k, carry):
        o_copy(k).wait_recv()
        return carry

    lax.fori_loop(1, n, wait_o, 0, unroll=unroll)
    got_max = inbox[:, rows_dev, :]
    got_sum = inbox[:, rows_dev + 1, :]
    far_max = jnp.max(got_max, axis=0, keepdims=True)
    got_f = jnp.exp(got_max - far_max)
    far_sum = jnp.sum(got_sum * got_f, axis=0, keepdims=True)
    mine = iota((rows_dev, rows), 1) == start + iota((rows_dev, rows), 0)

    def own_rows(x):
        return lane_sum(mine, jnp.broadcast_to(x, mine.shape))

    acc = jnp.zeros((rows_dev, proj.shape[1]), f32)
    for s in range(n):
        acc = acc + own_rows(got_f[s:s + 1]) * inbox[s, :rows_dev, :]
    far_max = own_rows(far_max)
    far_sum = own_rows(far_sum)
    own_score = own_score[:rows_dev]
    top = jnp.maximum(own_score, far_max)
    own_f = jnp.exp(own_score - top)
    far_f = jnp.exp(far_max - top)
    total = own_f + far_sum * far_f
    out[0] = ((own_f * new_out[:rows_dev] + acc * far_f) / total).astype(bf16)

    def wait_o_sent(k, carry):
        o_copy(k).wait_send()
        return carry

    lax.fori_loop(1, n, wait_o_sent, 0, unroll=unroll)


def shards(
    q_nope, q_rope, w_uk, w_uv, new_latent, shallow_cache, slot_positions, slab_map,
    deep_cache, deep_positions, lengths,
):
    n = lax.axis_size("holders")
    rows_dev, nope = q_nope.shape[1:]
    rope = q_rope.shape[2]
    slots, slab, width = shallow_cache.shape[1:]
    batch = new_latent.shape[1]
    value = w_uv.shape[3]
    deep_tok = deep_cache.shape[2]
    dma = pltpu.SemaphoreType.DMA
    any_spec = pl.BlockSpec(memory_space=pl.ANY)
    return pl.pallas_call(
        functools.partial(kernel, n, (rows_dev, slots, batch)),
        out_shape=jax.ShapeDtypeStruct((q_nope.shape[0], rows_dev, value), bf16),
        in_specs=[pl.BlockSpec(memory_space=pltpu.SMEM)] + [any_spec] * 10,
        out_specs=pl.BlockSpec(memory_space=pltpu.VMEM),
        scratch_shapes=[
            pltpu.VMEM((n, rows_dev, nope), bf16),
            pltpu.VMEM((n, rows_dev, rope), bf16),
            pltpu.VMEM((rows_dev, nope), bf16),
            pltpu.VMEM((rows_dev, rope), bf16),
            pltpu.VMEM(w_uk.shape[1:], bf16),
            pltpu.VMEM(w_uv.shape[1:], bf16),
            pltpu.VMEM((rows_dev,) + w_uk.shape[2:], bf16),
            pltpu.VMEM((rows_dev,) + w_uv.shape[2:], bf16),
            pltpu.VMEM(new_latent.shape, bf16),
            pltpu.VMEM((slots, slab, width), bf16),
            pltpu.VMEM((slots, slab), jnp.int32),
            pltpu.VMEM(slab_map.shape, jnp.int32),
            pltpu.VMEM((deep_tok, width), bf16),
            pltpu.VMEM((batch, deep_tok), jnp.int32),
            pltpu.VMEM((n * rows_dev, LATENT), bf16),
            pltpu.VMEM((slots * HEADS, LATENT), f32),
            pltpu.VMEM((n * rows_dev, value), f32),
            pltpu.VMEM((n, rows_dev + 2, value), f32),
            pltpu.VMEM((n, rows_dev + 2, value), f32),
            dma((13,)),
            dma((slots,)),
            dma((n,)),
            dma((n,)),
            dma((n,)),
            dma((n,)),
            dma((n,)),
            dma((n,)),
        ],
        compiler_params=pltpu.CompilerParams(
            collective_id=0, has_side_effects=True, vmem_limit_bytes=60 * 1024 * 1024
        ),
    )(
        lengths, q_nope, q_rope, w_uk, w_uv, new_latent, shallow_cache, slot_positions,
        slab_map, deep_cache, deep_positions,
    )


def solution(mesh):
    return jax.shard_map(
        shards,
        mesh=mesh,
        in_specs=(
            P(None, ("groups", "holders"), None),
            P(None, ("groups", "holders"), None),
            P(),
            P(),
            P(None, "groups", None),
            P(None, ("groups", "holders"), None, None),
            P(None, ("groups", "holders"), None),
            P(None, "groups"),
            P(None, "groups", None, None),
            P(None, "groups", None),
            P("groups"),
        ),
        out_specs=P(None, ("groups", "holders"), None),
        check_vma=False,
    )
```

```python
import functools

import jax
import jax.numpy as jnp
from jax import lax
from jax.experimental import pallas as pl
from jax.experimental.pallas import tpu as pltpu
from jax.sharding import PartitionSpec as P

HEADS = 16
LATENT = 512
SLABS_REQ = 16

score_scale = 192.0 ** (-0.5)
neg_fill = -1e30

f32 = jnp.float32
bf16 = jnp.bfloat16


def dot(a, b):
    return lax.dot_general(a, b, (((1,), (0,)), ((), ())), preferred_element_type=f32)


def dot_t(a, b):
    return lax.dot_general(a, b, (((1,), (1,)), ((), ())), preferred_element_type=f32)


def iota(shape, dim):
    return lax.broadcasted_iota(jnp.int32, shape, dim)


def lane_sum(mask, values):
    return jnp.sum(jnp.where(mask, values, jnp.zeros_like(values)), axis=1, keepdims=True)


def row_sum(mask, values):
    return jnp.sum(jnp.where(mask, values, jnp.zeros_like(values)), axis=0, keepdims=True)


def one_hot(mask):
    return jnp.where(mask, 1.0, 0.0).astype(bf16)


def kernel(
    n, dims,
    lengths, q_nope, q_rope, w_uk, w_uv, new_latent, cache, positions, slab_map,
    deep_cache, deep_positions,
    out,
    qn_all, qr_all, qn_deep, qr_deep, uk0, uv0, uk1, uv1, newlat, keys, pos, smap,
    dkeys, dpos, qlat, slot_out, proj, outbox, inbox,
    loc_sem, slab_sem, qn_send, qn_recv, qr_send, qr_recv, o_send, o_recv,
):
    rows_dev, slots, batch = dims
    rows = n * rows_dev
    srows = slots * HEADS
    me = lax.axis_index("holders")
    start = me * rows_dev
    head0 = lax.rem(start, HEADS)
    req = lax.div(start, HEADS)
    pad = max(8, rows_dev)
    unroll = n <= 16

    local = [
        (q_nope.at[0], qn_all.at[me]),
        (q_rope.at[0], qr_all.at[me]),
        (q_nope.at[1], qn_deep),
        (q_rope.at[1], qr_deep),
        (w_uk.at[1, pl.ds(head0, rows_dev)], uk1),
        (new_latent, newlat),
        (deep_positions.at[0], dpos),
        (deep_cache.at[0, req], dkeys),
        (w_uv.at[1, pl.ds(head0, rows_dev)], uv1),
        (slab_map, smap),
        (positions.at[0], pos),
        (w_uk.at[0], uk0),
        (w_uv.at[0], uv0),
    ]
    local = [pltpu.make_async_copy(s, d, loc_sem.at[i]) for i, (s, d) in enumerate(local)]
    slab_copies = [
        pltpu.make_async_copy(cache.at[0, j], keys.at[j], slab_sem.at[j]) for j in range(slots)
    ]

    for c in local[:2]:
        c.start()

    barrier = pltpu.get_barrier_semaphore()

    def greet(k, carry):
        peer = lax.rem(me + k, n)
        pl.semaphore_signal(
            barrier, inc=1, device_id={"holders": peer}, device_id_type=pl.DeviceIdType.MESH
        )
        return carry

    lax.fori_loop(1, n, greet, 0, unroll=unroll)
    for c in local[2:12]:
        c.start()
    for c in slab_copies:
        c.start()
    local[12].start()
    local[0].wait()
    local[1].wait()
    pl.semaphore_wait(barrier, n - 1)

    def remote(src, dst, ssem, rsem, k):
        peer = lax.rem(me + k, n)
        return pltpu.make_async_remote_copy(
            src_ref=src, dst_ref=dst, send_sem=ssem.at[k], recv_sem=rsem.at[k],
            device_id={"holders": peer}, device_id_type=pl.DeviceIdType.MESH,
        )

    def q_copies(k):
        return (
            remote(qn_all.at[me], qn_all.at[me], qn_send, qn_recv, k),
            remote(qr_all.at[me], qr_all.at[me], qr_send, qr_recv, k),
        )

    def send_q(k, carry):
        for c in q_copies(k):
            c.start()
        return carry

    lax.fori_loop(1, n, send_q, 0, unroll=unroll)

    def widen(x):
        if x.shape[0] < pad:
            x = jnp.concatenate([x] * (pad // x.shape[0]), axis=0)
        return x

    own_row = lax.rem(iota((pad, 1), 0), rows_dev)

    def per_head(x, head_of):
        acc = None
        for i in range(rows_dev):
            part = dot(x, head_of(i))
            acc = part if acc is None else jnp.where(own_row == i, part, acc)
        return acc

    for c in local[2:9]:
        c.wait()
    pick = iota((batch, newlat.shape[2]), 0) == req
    new1 = row_sum(pick, newlat[1].astype(f32))
    new0 = row_sum(pick, newlat[0].astype(f32))
    qn1 = widen(qn_deep[...].astype(f32)).astype(bf16)
    qr1 = widen(qr_deep[...].astype(f32)).astype(bf16)
    ql1 = per_head(qn1, lambda i: uk1[i]).astype(bf16)
    score = (dot(ql1, dkeys[:LATENT]) + dot(qr1, dkeys[LATENT:])) * score_scale
    where1 = row_sum(iota(dpos.shape, 0) == req, dpos[...])
    live = where1 < lengths[req]
    own_max = jnp.max(jnp.where(live, score, neg_fill), axis=1, keepdims=True)
    weight = jnp.where(live, jnp.exp(jnp.where(live, score - own_max, 0.0)), 0.0).astype(bf16)
    own_sum = jnp.sum(weight.astype(f32), axis=1, keepdims=True)
    own_out = dot_t(weight, dkeys[:LATENT])

    def own_scores(ql, qr, new):
        lat = jnp.sum(ql.astype(f32) * new[:, :LATENT], axis=1, keepdims=True)
        rot = jnp.sum(qr.astype(f32) * new[:, LATENT:], axis=1, keepdims=True)
        return (lat + rot) * score_scale

    own_score = own_scores(ql1, qr1, new1)
    top = jnp.maximum(own_score, own_max)
    own_f = jnp.exp(own_score - top)
    far_f = jnp.exp(own_max - top)
    total = own_f + own_sum * far_f
    mixed = ((own_f * new1[:, :LATENT] + own_out * far_f) / total).astype(bf16)
    attended1 = per_head(mixed, lambda i: uv1[i])
    out[1] = attended1[:rows_dev].astype(bf16)

    for c in local[9:12]:
        c.wait()
    r_s = iota((srows, rows), 0)
    c_s = iota((srows, rows), 1)
    found = smap[...] == me * slots + lax.div(iota((srows, smap.shape[1]), 0), HEADS)
    req_col = lane_sum(found, lax.div(iota((srows, smap.shape[1]), 1), SLABS_REQ))
    len_col = jnp.zeros((srows, 1), jnp.int32)
    for b in range(batch):
        len_col = jnp.where(req_col == b, lengths[b], len_col)
    sel_bh = (lax.div(c_s, HEADS) == req_col) & (lax.rem(c_s, HEADS) == lax.rem(r_s, HEADS))
    sel_hb = (lax.rem(c_s, batch) == req_col) & (lax.div(c_s, batch) == lax.rem(r_s, HEADS))
    sel_bh, sel_hb = one_hot(sel_bh), one_hot(sel_hb)
    r_q = iota((rows, rows), 0)
    c_q = iota((rows, rows), 1)
    perm = (lax.rem(r_q, batch) == lax.div(c_q, HEADS)) & (lax.div(r_q, batch) == lax.rem(c_q, HEADS))
    eye = iota((srows, srows), 0) == iota((srows, srows), 1)
    req_row = row_sum(eye, jnp.broadcast_to(req_col, eye.shape))
    r_t = iota((rows, srows), 0)
    c_t = iota((rows, srows), 1)
    back = (lax.div(r_t, batch) == lax.rem(c_t, HEADS)) & (lax.rem(r_t, batch) == req_row)

    def wait_q(k, carry):
        for c in q_copies(k):
            c.wait_recv()
        return carry

    lax.fori_loop(1, n, wait_q, 0, unroll=unroll)
    qn = qn_all[...].astype(f32).reshape(rows, qn_all.shape[2]).astype(bf16)
    qr = qr_all[...].astype(f32).reshape(rows, qr_all.shape[2]).astype(bf16)
    qn_hb = dot(one_hot(perm), qn)
    for h in range(0, HEADS, 2):
        two = [
            dot(qn_hb[g * batch:(g + 1) * batch].astype(bf16), uk0[g]) for g in (h, h + 1)
        ]
        qlat[h * batch:(h + 2) * batch, :] = jnp.concatenate(two, axis=0).astype(bf16)
    q_slot = dot(sel_hb, qlat[...]).astype(bf16)
    r_slot = dot(sel_bh, qr).astype(bf16)

    maxes, sums = [], []
    for j in range(slots):
        at = slice(j * HEADS, (j + 1) * HEADS)
        slab_copies[j].wait()
        score = (
            dot(q_slot[at], keys[j, :LATENT]) + dot(r_slot[at], keys[j, LATENT:])
        ) * score_scale
        live = pos[j:j + 1, :] < len_col[at]
        block_max = jnp.max(jnp.where(live, score, neg_fill), axis=1, keepdims=True)
        weight = jnp.where(
            live, jnp.exp(jnp.where(live, score - block_max, 0.0)), 0.0
        ).astype(bf16)
        maxes.append(block_max)
        sums.append(jnp.sum(weight.astype(f32), axis=1, keepdims=True))
        slot_out[at, :] = dot_t(weight, keys[j, :LATENT])
    slot_max = jnp.concatenate(maxes, axis=0)
    slot_sum = jnp.concatenate(sums, axis=0)

    max_row = row_sum(eye, jnp.broadcast_to(slot_max, eye.shape))
    sum_row = row_sum(eye, jnp.broadcast_to(slot_sum, eye.shape))
    dense_max = jnp.max(jnp.where(back, max_row, neg_fill), axis=1, keepdims=True)
    factor_row = jnp.exp(max_row - row_sum(back, jnp.broadcast_to(dense_max, back.shape)))
    dense_sum = lane_sum(back, jnp.broadcast_to(sum_row * factor_row, back.shape))
    factor_col = lane_sum(eye, jnp.broadcast_to(factor_row, eye.shape))
    scaled = (slot_out[...] * factor_col).astype(bf16)
    dense = dot(one_hot(back), scaled)
    local[12].wait()
    for h in range(HEADS):
        part = dot(dense[h * batch:(h + 1) * batch].astype(bf16), uv0[h])
        proj[pl.ds(h, batch, stride=HEADS), :] = part
    outbox[:, :rows_dev, :] = proj[...].reshape(n, rows_dev, proj.shape[1])
    stat_max = row_sum(perm, jnp.broadcast_to(dense_max, perm.shape))
    stat_sum = row_sum(perm, jnp.broadcast_to(dense_sum, perm.shape))
    stats = jnp.concatenate([stat_max, stat_sum], axis=0)
    outbox[:, rows_dev:, :] = jnp.broadcast_to(stats[None], (n,) + stats.shape)
    inbox[me] = outbox[me]

    def o_copy(k):
        return remote(outbox.at[lax.rem(me + k, n)], inbox.at[me], o_send, o_recv, k)

    def send_o(k, carry):
        o_copy(k).start()
        return carry

    lax.fori_loop(1, n, send_o, 0, unroll=unroll)

    qn0 = widen(qn_all[me].astype(f32)).astype(bf16)
    qr0 = widen(qr_all[me].astype(f32)).astype(bf16)
    ql0 = per_head(qn0, lambda i: uk0[head0 + i]).astype(bf16)
    own_score = own_scores(ql0, qr0, new0)
    new_in = jnp.broadcast_to(new0[:, :LATENT], (pad, LATENT)).astype(bf16)
    new_out = per_head(new_in, lambda i: uv0[head0 + i])

    def wait_sent(k, carry):
        for c in q_copies(k):
            c.wait_send()
        return carry

    lax.fori_loop(1, n, wait_sent, 0, unroll=unroll)

    def wait_o(k, carry):
        o_copy(k).wait_recv()
        return carry

    lax.fori_loop(1, n, wait_o, 0, unroll=unroll)
    got_max = inbox[:, rows_dev, :]
    got_sum = inbox[:, rows_dev + 1, :]
    far_max = jnp.max(got_max, axis=0, keepdims=True)
    got_f = jnp.exp(got_max - far_max)
    far_sum = jnp.sum(got_sum * got_f, axis=0, keepdims=True)
    mine = iota((rows_dev, rows), 1) == start + iota((rows_dev, rows), 0)

    def own_rows(x):
        return lane_sum(mine, jnp.broadcast_to(x, mine.shape))

    acc = jnp.zeros((rows_dev, proj.shape[1]), f32)
    for s in range(n):
        acc = acc + own_rows(got_f[s:s + 1]) * inbox[s, :rows_dev, :]
    far_max = own_rows(far_max)
    far_sum = own_rows(far_sum)
    own_score = own_score[:rows_dev]
    top = jnp.maximum(own_score, far_max)
    own_f = jnp.exp(own_score - top)
    far_f = jnp.exp(far_max - top)
    total = own_f + far_sum * far_f
    out[0] = ((own_f * new_out[:rows_dev] + acc * far_f) / total).astype(bf16)

    def wait_o_sent(k, carry):
        o_copy(k).wait_send()
        return carry

    lax.fori_loop(1, n, wait_o_sent, 0, unroll=unroll)


def shards(
    q_nope, q_rope, w_uk, w_uv, new_latent, shallow_cache, slot_positions, slab_map,
    deep_cache, deep_positions, lengths,
):
    n = lax.axis_size("holders")
    rows_dev, nope = q_nope.shape[1:]
    rope = q_rope.shape[2]
    slots, slab, width = shallow_cache.shape[1:]
    batch = new_latent.shape[1]
    value = w_uv.shape[3]
    deep_tok = deep_cache.shape[2]
    dma = pltpu.SemaphoreType.DMA
    any_spec = pl.BlockSpec(memory_space=pl.ANY)
    return pl.pallas_call(
        functools.partial(kernel, n, (rows_dev, slots, batch)),
        out_shape=jax.ShapeDtypeStruct((q_nope.shape[0], rows_dev, value), bf16),
        in_specs=[pl.BlockSpec(memory_space=pltpu.SMEM)] + [any_spec] * 10,
        out_specs=pl.BlockSpec(memory_space=pltpu.VMEM),
        scratch_shapes=[
            pltpu.VMEM((n, rows_dev, nope), bf16),
            pltpu.VMEM((n, rows_dev, rope), bf16),
            pltpu.VMEM((rows_dev, nope), bf16),
            pltpu.VMEM((rows_dev, rope), bf16),
            pltpu.VMEM(w_uk.shape[1:], bf16),
            pltpu.VMEM(w_uv.shape[1:], bf16),
            pltpu.VMEM((rows_dev,) + w_uk.shape[2:], bf16),
            pltpu.VMEM((rows_dev,) + w_uv.shape[2:], bf16),
            pltpu.VMEM(new_latent.shape, bf16),
            pltpu.VMEM((slots, width, slab), bf16),
            pltpu.VMEM((slots, slab), jnp.int32),
            pltpu.VMEM(slab_map.shape, jnp.int32),
            pltpu.VMEM((width, deep_tok), bf16),
            pltpu.VMEM((batch, deep_tok), jnp.int32),
            pltpu.VMEM((n * rows_dev, LATENT), bf16),
            pltpu.VMEM((slots * HEADS, LATENT), f32),
            pltpu.VMEM((n * rows_dev, value), f32),
            pltpu.VMEM((n, rows_dev + 2, value), f32),
            pltpu.VMEM((n, rows_dev + 2, value), f32),
            dma((13,)),
            dma((slots,)),
            dma((n,)),
            dma((n,)),
            dma((n,)),
            dma((n,)),
            dma((n,)),
            dma((n,)),
        ],
        compiler_params=pltpu.CompilerParams(
            collective_id=0, has_side_effects=True, vmem_limit_bytes=60 * 1024 * 1024
        ),
    )(
        lengths, q_nope, q_rope, w_uk, w_uv, new_latent, jnp.swapaxes(shallow_cache, 2, 3),
        slot_positions, slab_map, jnp.swapaxes(deep_cache, 2, 3), deep_positions,
    )


def solution(mesh):
    return jax.shard_map(
        shards,
        mesh=mesh,
        in_specs=(
            P(None, ("groups", "holders"), None),
            P(None, ("groups", "holders"), None),
            P(),
            P(),
            P(None, "groups", None),
            P(None, ("groups", "holders"), None, None),
            P(None, ("groups", "holders"), None),
            P(None, "groups"),
            P(None, "groups", None, None),
            P(None, "groups", None),
            P("groups"),
        ),
        out_specs=P(None, ("groups", "holders"), None),
        check_vma=False,
    )
```

```python
import functools

import jax
import jax.numpy as jnp
from jax import lax
from jax.experimental import pallas as pl
from jax.experimental.pallas import tpu as pltpu
from jax.sharding import PartitionSpec as P

HEADS = 16
LATENT = 512
SLABS_REQ = 16

score_scale = 192.0 ** (-0.5)
neg_fill = -1e30

f32 = jnp.float32
bf16 = jnp.bfloat16


def dot(a, b):
    return lax.dot_general(a, b, (((1,), (0,)), ((), ())), preferred_element_type=f32)


def dot_t(a, b):
    return lax.dot_general(a, b, (((1,), (1,)), ((), ())), preferred_element_type=f32)


def iota(shape, dim):
    return lax.broadcasted_iota(jnp.int32, shape, dim)


def lane_sum(mask, values):
    return jnp.sum(jnp.where(mask, values, jnp.zeros_like(values)), axis=1, keepdims=True)


def row_sum(mask, values):
    return jnp.sum(jnp.where(mask, values, jnp.zeros_like(values)), axis=0, keepdims=True)


def one_hot(mask):
    return jnp.where(mask, 1.0, 0.0).astype(bf16)


def kernel(
    n, dims,
    lengths, q_nope, q_rope, w_uk, w_uv, new_latent, cache, positions, slab_map,
    deep_cache, deep_positions,
    out,
    qn_all, qr_all, qn_deep, qr_deep, uk0, uv0, uk1, uv1, newlat, keys, pos, smap,
    dkeys, dpos, qlat, score, dead, proj, outbox, inbox,
    loc_sem, slab_sem, qn_send, qn_recv, qr_send, qr_recv, o_send, o_recv,
):
    rows_dev, slots, batch = dims
    rows = n * rows_dev
    srows = slots * HEADS
    me = lax.axis_index("holders")
    start = me * rows_dev
    head0 = lax.rem(start, HEADS)
    req = lax.div(start, HEADS)
    pad = max(8, rows_dev)
    unroll = n <= 16
    lanes = qlat.shape[2]

    local = [
        (q_nope.at[0], qn_all.at[me]),
        (q_rope.at[0], qr_all.at[me]),
        (q_nope.at[1], qn_deep),
        (q_rope.at[1], qr_deep),
        (w_uk.at[1, pl.ds(head0, rows_dev)], uk1),
        (new_latent, newlat),
        (deep_positions.at[0], dpos),
        (deep_cache.at[0, req], dkeys),
        (w_uv.at[1, pl.ds(head0, rows_dev)], uv1),
        (slab_map, smap),
        (positions.at[0], pos),
        (w_uk.at[0], uk0),
        (w_uv.at[0], uv0),
    ]
    local = [pltpu.make_async_copy(s, d, loc_sem.at[i]) for i, (s, d) in enumerate(local)]
    slab_copies = [
        pltpu.make_async_copy(cache.at[0, j], keys.at[j], slab_sem.at[j]) for j in range(slots)
    ]

    for c in local[:2]:
        c.start()

    barrier = pltpu.get_barrier_semaphore()

    def greet(k, carry):
        peer = lax.rem(me + k, n)
        pl.semaphore_signal(
            barrier, inc=1, device_id={"holders": peer}, device_id_type=pl.DeviceIdType.MESH
        )
        return carry

    lax.fori_loop(1, n, greet, 0, unroll=unroll)
    for c in local[2:12]:
        c.start()
    for c in slab_copies:
        c.start()
    local[12].start()
    local[0].wait()
    local[1].wait()
    pl.semaphore_wait(barrier, n - 1)

    def remote(src, dst, ssem, rsem, k):
        peer = lax.rem(me + k, n)
        return pltpu.make_async_remote_copy(
            src_ref=src, dst_ref=dst, send_sem=ssem.at[k], recv_sem=rsem.at[k],
            device_id={"holders": peer}, device_id_type=pl.DeviceIdType.MESH,
        )

    def q_copies(k):
        return (
            remote(qn_all.at[me], qn_all.at[me], qn_send, qn_recv, k),
            remote(qr_all.at[me], qr_all.at[me], qr_send, qr_recv, k),
        )

    def send_q(k, carry):
        for c in q_copies(k):
            c.start()
        return carry

    lax.fori_loop(1, n, send_q, 0, unroll=unroll)

    def widen(x):
        if x.shape[0] < pad:
            x = jnp.concatenate([x] * (pad // x.shape[0]), axis=0)
        return x

    own_row = lax.rem(iota((pad, 1), 0), rows_dev)

    def per_head(x, head_of):
        acc = None
        for i in range(rows_dev):
            part = dot(x, head_of(i))
            acc = part if acc is None else jnp.where(own_row == i, part, acc)
        return acc

    for c in local[2:9]:
        c.wait()
    pick = iota((batch, newlat.shape[2]), 0) == req
    new1 = row_sum(pick, newlat[1].astype(f32))
    new0 = row_sum(pick, newlat[0].astype(f32))
    qn1 = widen(qn_deep[...].astype(f32)).astype(bf16)
    qr1 = widen(qr_deep[...].astype(f32)).astype(bf16)
    ql1 = per_head(qn1, lambda i: uk1[i]).astype(bf16)
    score1 = (dot(ql1, dkeys[:LATENT]) + dot(qr1, dkeys[LATENT:])) * score_scale
    where1 = row_sum(iota(dpos.shape, 0) == req, dpos[...])
    live = where1 < lengths[req]
    own_max = jnp.max(jnp.where(live, score1, neg_fill), axis=1, keepdims=True)
    weight = jnp.where(live, jnp.exp(jnp.where(live, score1 - own_max, 0.0)), 0.0).astype(bf16)
    own_sum = jnp.sum(weight.astype(f32), axis=1, keepdims=True)
    own_out = dot_t(weight, dkeys[:LATENT])

    def own_scores(ql, qr, new):
        lat = jnp.sum(ql.astype(f32) * new[:, :LATENT], axis=1, keepdims=True)
        rot = jnp.sum(qr.astype(f32) * new[:, LATENT:], axis=1, keepdims=True)
        return (lat + rot) * score_scale

    own_score = own_scores(ql1, qr1, new1)
    top = jnp.maximum(own_score, own_max)
    own_f = jnp.exp(own_score - top)
    far_f = jnp.exp(own_max - top)
    total = own_f + own_sum * far_f
    mixed = ((own_f * new1[:, :LATENT] + own_out * far_f) / total).astype(bf16)
    attended1 = per_head(mixed, lambda i: uv1[i])
    out[1] = attended1[:rows_dev].astype(bf16)

    for c in local[9:12]:
        c.wait()
    r_s = iota((srows, rows), 0)
    c_s = iota((srows, rows), 1)
    own_slots = me * slots
    entry = lax.div(iota((srows, smap.shape[1]), 1), SLABS_REQ)
    map_row = iota((srows, smap.shape[1]), 0)
    by_slot = lane_sum(smap[...] == own_slots + lax.div(map_row, HEADS), entry)
    by_head = lane_sum(smap[...] == own_slots + lax.rem(map_row, slots), entry)
    len_col = jnp.zeros((srows, 1), jnp.int32)
    for b in range(batch):
        len_col = jnp.where(by_slot == b, lengths[b], len_col)
    c_req, c_head = lax.div(c_s, HEADS), lax.rem(c_s, HEADS)
    sel = (c_req == by_slot) & (c_head == lax.rem(r_s, HEADS))
    sel_hot = one_hot(sel)
    sel_head = one_hot((c_req == by_head) & (c_head == lax.div(r_s, slots)))
    eye = iota((srows, srows), 0) == iota((srows, srows), 1)
    req_row = row_sum(eye, jnp.broadcast_to(by_slot, eye.shape))
    r_t = iota((rows, srows), 0)
    c_t = iota((rows, srows), 1)
    back = one_hot(
        (lax.div(r_t, batch) == lax.rem(c_t, HEADS)) & (lax.rem(r_t, batch) == req_row)
    )
    live = jnp.concatenate(
        [pos[j:j + 1, :] < len_col[j * HEADS:(j + 1) * HEADS] for j in range(slots)], axis=0
    )
    dead[...] = jnp.where(live, 0.0, -jnp.inf)
    for c in slab_copies:
        c.wait()
    local[12].wait()

    def wait_q(k, carry):
        for c in q_copies(k):
            c.wait_recv()
        return carry

    lax.fori_loop(1, n, wait_q, 0, unroll=unroll)
    qn = qn_all[...].astype(f32).reshape(rows, qn_all.shape[2]).astype(bf16)
    qr = qr_all[...].astype(f32).reshape(rows, qr_all.shape[2]).astype(bf16)
    qn_head = dot(sel_head, qn)
    for h in range(HEADS):
        at = slice(h * slots, (h + 1) * slots)
        full = dot(qn_head[at].astype(bf16), uk0[h])
        for t in range(qlat.shape[0]):
            qlat[t, at, :] = full[:, t * lanes:(t + 1) * lanes]
    r_slot = dot(sel_hot, qr).astype(bf16)

    for j in range(slots):
        at = slice(j * HEADS, (j + 1) * HEADS)
        q_slot = jnp.concatenate(
            [qlat[t, pl.ds(j, HEADS, stride=slots), :] for t in range(qlat.shape[0])], axis=1
        ).astype(bf16)
        score[at, :] = dot(q_slot, keys[j, :LATENT]) + dot(r_slot[at], keys[j, LATENT:])
    masked = score[...] * score_scale + dead[...]
    slot_max = jnp.max(masked, axis=1, keepdims=True)
    stat_max = jnp.max(jnp.where(sel, slot_max, neg_fill), axis=0, keepdims=True)
    group_max = jnp.max(jnp.where(sel, stat_max, neg_fill), axis=1, keepdims=True)
    weight = jnp.exp(masked - group_max).astype(bf16)
    slot_sum = jnp.sum(weight.astype(f32), axis=1, keepdims=True)
    stat_sum = row_sum(sel, jnp.broadcast_to(slot_sum, sel.shape))
    parts = [
        dot_t(weight[j * HEADS:(j + 1) * HEADS], keys[j, :LATENT]).astype(bf16)
        for j in range(slots)
    ]

    dense = dot(back, jnp.concatenate(parts, axis=0))
    for h in range(HEADS):
        part = dot(dense[h * batch:(h + 1) * batch].astype(bf16), uv0[h])
        proj[pl.ds(h, batch, stride=HEADS), :] = part
    outbox[:, :rows_dev, :] = proj[...].reshape(n, rows_dev, proj.shape[1])
    stats = jnp.concatenate([stat_max, stat_sum], axis=0)
    outbox[:, rows_dev:, :] = jnp.broadcast_to(stats[None], (n,) + stats.shape)
    inbox[me] = outbox[me]

    def o_copy(k):
        return remote(outbox.at[lax.rem(me + k, n)], inbox.at[me], o_send, o_recv, k)

    def send_o(k, carry):
        o_copy(k).start()
        return carry

    lax.fori_loop(1, n, send_o, 0, unroll=unroll)

    qn0 = widen(qn_all[me].astype(f32)).astype(bf16)
    qr0 = widen(qr_all[me].astype(f32)).astype(bf16)
    ql0 = per_head(qn0, lambda i: uk0[head0 + i]).astype(bf16)
    own_score = own_scores(ql0, qr0, new0)
    new_in = jnp.broadcast_to(new0[:, :LATENT], (pad, LATENT)).astype(bf16)
    new_out = per_head(new_in, lambda i: uv0[head0 + i])

    def wait_sent(k, carry):
        for c in q_copies(k):
            c.wait_send()
        return carry

    lax.fori_loop(1, n, wait_sent, 0, unroll=unroll)

    def wait_o(k, carry):
        o_copy(k).wait_recv()
        return carry

    lax.fori_loop(1, n, wait_o, 0, unroll=unroll)
    got_max = inbox[:, rows_dev, :]
    got_sum = inbox[:, rows_dev + 1, :]
    far_max = jnp.max(got_max, axis=0, keepdims=True)
    got_f = jnp.exp(got_max - far_max)
    far_sum = jnp.sum(got_sum * got_f, axis=0, keepdims=True)
    mine = iota((rows_dev, rows), 1) == start + iota((rows_dev, rows), 0)

    def own_rows(x):
        return lane_sum(mine, jnp.broadcast_to(x, mine.shape))

    acc = jnp.zeros((rows_dev, proj.shape[1]), f32)
    for s in range(n):
        acc = acc + own_rows(got_f[s:s + 1]) * inbox[s, :rows_dev, :]
    far_max = own_rows(far_max)
    far_sum = own_rows(far_sum)
    own_score = own_score[:rows_dev]
    top = jnp.maximum(own_score, far_max)
    own_f = jnp.exp(own_score - top)
    far_f = jnp.exp(far_max - top)
    total = own_f + far_sum * far_f
    out[0] = ((own_f * new_out[:rows_dev] + acc * far_f) / total).astype(bf16)

    def wait_o_sent(k, carry):
        o_copy(k).wait_send()
        return carry

    lax.fori_loop(1, n, wait_o_sent, 0, unroll=unroll)


def shards(
    q_nope, q_rope, w_uk, w_uv, new_latent, shallow_cache, slot_positions, slab_map,
    deep_cache, deep_positions, lengths,
):
    n = lax.axis_size("holders")
    rows_dev, nope = q_nope.shape[1:]
    rope = q_rope.shape[2]
    slots, slab, width = shallow_cache.shape[1:]
    batch = new_latent.shape[1]
    value = w_uv.shape[3]
    deep_tok = deep_cache.shape[2]
    dma = pltpu.SemaphoreType.DMA
    any_spec = pl.BlockSpec(memory_space=pl.ANY)
    return pl.pallas_call(
        functools.partial(kernel, n, (rows_dev, slots, batch)),
        out_shape=jax.ShapeDtypeStruct((q_nope.shape[0], rows_dev, value), bf16),
        in_specs=[pl.BlockSpec(memory_space=pltpu.SMEM)] + [any_spec] * 10,
        out_specs=pl.BlockSpec(memory_space=pltpu.VMEM),
        scratch_shapes=[
            pltpu.VMEM((n, rows_dev, nope), bf16),
            pltpu.VMEM((n, rows_dev, rope), bf16),
            pltpu.VMEM((rows_dev, nope), bf16),
            pltpu.VMEM((rows_dev, rope), bf16),
            pltpu.VMEM(w_uk.shape[1:], bf16),
            pltpu.VMEM(w_uv.shape[1:], bf16),
            pltpu.VMEM((rows_dev,) + w_uk.shape[2:], bf16),
            pltpu.VMEM((rows_dev,) + w_uv.shape[2:], bf16),
            pltpu.VMEM(new_latent.shape, bf16),
            pltpu.VMEM((slots, width, slab), bf16),
            pltpu.VMEM((slots, slab), jnp.int32),
            pltpu.VMEM(slab_map.shape, jnp.int32),
            pltpu.VMEM((width, deep_tok), bf16),
            pltpu.VMEM((batch, deep_tok), jnp.int32),
            pltpu.VMEM((LATENT // 128, slots * HEADS, 128), f32),
            pltpu.VMEM((slots * HEADS, slab), f32),
            pltpu.VMEM((slots * HEADS, slab), f32),
            pltpu.VMEM((n * rows_dev, value), f32),
            pltpu.VMEM((n, rows_dev + 2, value), f32),
            pltpu.VMEM((n, rows_dev + 2, value), f32),
            dma((13,)),
            dma((slots,)),
            dma((n,)),
            dma((n,)),
            dma((n,)),
            dma((n,)),
            dma((n,)),
            dma((n,)),
        ],
        compiler_params=pltpu.CompilerParams(
            collective_id=0, has_side_effects=True, vmem_limit_bytes=60 * 1024 * 1024
        ),
    )(
        lengths, q_nope, q_rope, w_uk, w_uv, new_latent, jnp.swapaxes(shallow_cache, 2, 3),
        slot_positions, slab_map, jnp.swapaxes(deep_cache, 2, 3), deep_positions,
    )


def solution(mesh):
    return jax.shard_map(
        shards,
        mesh=mesh,
        in_specs=(
            P(None, ("groups", "holders"), None),
            P(None, ("groups", "holders"), None),
            P(),
            P(),
            P(None, "groups", None),
            P(None, ("groups", "holders"), None, None),
            P(None, ("groups", "holders"), None),
            P(None, "groups"),
            P(None, "groups", None, None),
            P(None, "groups", None),
            P("groups"),
        ),
        out_specs=P(None, ("groups", "holders"), None),
        check_vma=False,
    )
```

```python
import functools

import jax
import jax.numpy as jnp
from jax import lax
from jax.experimental import pallas as pl
from jax.experimental.pallas import tpu as pltpu
from jax.sharding import PartitionSpec as P

HEADS = 16
LATENT = 512
SLABS_REQ = 16

score_scale = 192.0 ** (-0.5)
neg_fill = -1e30

f32 = jnp.float32
bf16 = jnp.bfloat16


def dot(a, b):
    return lax.dot_general(a, b, (((1,), (0,)), ((), ())), preferred_element_type=f32)


def dot_t(a, b):
    return lax.dot_general(a, b, (((1,), (1,)), ((), ())), preferred_element_type=f32)


def iota(shape, dim):
    return lax.broadcasted_iota(jnp.int32, shape, dim)


def lane_sum(mask, values):
    return jnp.sum(jnp.where(mask, values, jnp.zeros_like(values)), axis=1, keepdims=True)


def row_sum(mask, values):
    return jnp.sum(jnp.where(mask, values, jnp.zeros_like(values)), axis=0, keepdims=True)


def one_hot(mask):
    return jnp.where(mask, 1.0, 0.0).astype(bf16)


def kernel(
    n, dims,
    lengths, q_nope, q_rope, w_uk, w_uv, new_latent, cache, positions, slab_map,
    deep_cache, deep_positions,
    out,
    qn_all, qr_all, qn_deep, qr_deep, uk0, uv0, uk1, uv1, newlat, keys, pos, smap,
    dkeys, dpos, qlat, score, dead, proj, outbox, inbox, stats,
    loc_sem, slab_sem, qn_send, qn_recv, qr_send, qr_recv, o_send, o_recv, st_send, st_recv,
):
    rows_dev, slots, batch = dims
    rows = n * rows_dev
    srows = slots * HEADS
    me = lax.axis_index("holders")
    start = me * rows_dev
    head0 = lax.rem(start, HEADS)
    req = lax.div(start, HEADS)
    pad = max(8, rows_dev)
    unroll = n <= 16

    def spread(body):
        if unroll:
            for k in sorted(range(1, n), key=lambda k: -abs(k - n // 2)):
                body(k, 0)
        else:
            lax.fori_loop(1, n, body, 0)

    lanes = qlat.shape[2]

    local = [
        (q_nope.at[0], qn_all.at[me]),
        (q_rope.at[0], qr_all.at[me]),
        (q_nope.at[1], qn_deep),
        (q_rope.at[1], qr_deep),
        (w_uk.at[1, pl.ds(head0, rows_dev)], uk1),
        (new_latent, newlat),
        (deep_positions.at[0], dpos),
        (deep_cache.at[0, req], dkeys),
        (w_uv.at[1, pl.ds(head0, rows_dev)], uv1),
        (slab_map, smap),
        (positions.at[0], pos),
        (w_uk.at[0], uk0),
        (w_uv.at[0], uv0),
    ]
    local = [pltpu.make_async_copy(s, d, loc_sem.at[i]) for i, (s, d) in enumerate(local)]
    slab_copies = [
        pltpu.make_async_copy(cache.at[0, j], keys.at[j], slab_sem.at[j]) for j in range(slots)
    ]

    for c in local[:2]:
        c.start()

    barrier = pltpu.get_barrier_semaphore()

    def greet(k, carry):
        peer = lax.rem(me + k, n)
        pl.semaphore_signal(
            barrier, inc=1, device_id={"holders": peer}, device_id_type=pl.DeviceIdType.MESH
        )
        return carry

    spread(greet)
    for c in local[2:12]:
        c.start()
    for c in slab_copies:
        c.start()
    local[12].start()
    local[0].wait()
    local[1].wait()
    pl.semaphore_wait(barrier, n - 1)

    def remote(src, dst, ssem, rsem, k):
        peer = lax.rem(me + k, n)
        return pltpu.make_async_remote_copy(
            src_ref=src, dst_ref=dst, send_sem=ssem.at[k], recv_sem=rsem.at[k],
            device_id={"holders": peer}, device_id_type=pl.DeviceIdType.MESH,
        )

    def q_copies(k):
        return (
            remote(qn_all.at[me], qn_all.at[me], qn_send, qn_recv, k),
            remote(qr_all.at[me], qr_all.at[me], qr_send, qr_recv, k),
        )

    def send_q(k, carry):
        for c in q_copies(k):
            c.start()
        return carry

    spread(send_q)

    def widen(x):
        if x.shape[0] < pad:
            x = jnp.concatenate([x] * (pad // x.shape[0]), axis=0)
        return x

    own_row = lax.rem(iota((pad, 1), 0), rows_dev)

    def per_head(x, head_of):
        acc = None
        for i in range(rows_dev):
            part = dot(x, head_of(i))
            acc = part if acc is None else jnp.where(own_row == i, part, acc)
        return acc

    for c in local[2:9]:
        c.wait()
    pick = iota((batch, newlat.shape[2]), 0) == req
    new1 = row_sum(pick, newlat[1].astype(f32))
    new0 = row_sum(pick, newlat[0].astype(f32))
    qn1 = widen(qn_deep[...].astype(f32)).astype(bf16)
    qr1 = widen(qr_deep[...].astype(f32)).astype(bf16)
    ql1 = per_head(qn1, lambda i: uk1[i]).astype(bf16)
    score1 = (dot(ql1, dkeys[:LATENT]) + dot(qr1, dkeys[LATENT:])) * score_scale
    where1 = row_sum(iota(dpos.shape, 0) == req, dpos[...])
    live = where1 < lengths[req]
    own_max = jnp.max(jnp.where(live, score1, neg_fill), axis=1, keepdims=True)
    weight = jnp.where(live, jnp.exp(jnp.where(live, score1 - own_max, 0.0)), 0.0).astype(bf16)
    own_sum = jnp.sum(weight.astype(f32), axis=1, keepdims=True)
    own_out = dot_t(weight, dkeys[:LATENT])

    def own_scores(ql, qr, new):
        lat = jnp.sum(ql.astype(f32) * new[:, :LATENT], axis=1, keepdims=True)
        rot = jnp.sum(qr.astype(f32) * new[:, LATENT:], axis=1, keepdims=True)
        return (lat + rot) * score_scale

    own_score = own_scores(ql1, qr1, new1)
    top = jnp.maximum(own_score, own_max)
    own_f = jnp.exp(own_score - top)
    far_f = jnp.exp(own_max - top)
    total = own_f + own_sum * far_f
    mixed = ((own_f * new1[:, :LATENT] + own_out * far_f) / total).astype(bf16)
    attended1 = per_head(mixed, lambda i: uv1[i])
    out[1] = attended1[:rows_dev].astype(bf16)

    for c in local[9:12]:
        c.wait()
    r_s = iota((srows, rows), 0)
    c_s = iota((srows, rows), 1)
    own_slots = me * slots
    entry = lax.div(iota((srows, smap.shape[1]), 1), SLABS_REQ)
    map_row = iota((srows, smap.shape[1]), 0)
    by_slot = lane_sum(smap[...] == own_slots + lax.div(map_row, HEADS), entry)
    by_head = lane_sum(smap[...] == own_slots + lax.rem(map_row, slots), entry)
    len_col = jnp.zeros((srows, 1), jnp.int32)
    for b in range(batch):
        len_col = jnp.where(by_slot == b, lengths[b], len_col)
    c_req, c_head = lax.div(c_s, HEADS), lax.rem(c_s, HEADS)
    sel = (c_req == by_slot) & (c_head == lax.rem(r_s, HEADS))
    sel_hot = one_hot(sel)
    sel_head = one_hot((c_req == by_head) & (c_head == lax.div(r_s, slots)))
    eye = iota((srows, srows), 0) == iota((srows, srows), 1)
    req_row = row_sum(eye, jnp.broadcast_to(by_slot, eye.shape))
    r_t = iota((rows, srows), 0)
    c_t = iota((rows, srows), 1)
    back = one_hot(
        (lax.div(r_t, batch) == lax.rem(c_t, HEADS)) & (lax.rem(r_t, batch) == req_row)
    )
    live = jnp.concatenate(
        [pos[j:j + 1, :] < len_col[j * HEADS:(j + 1) * HEADS] for j in range(slots)], axis=0
    )
    dead[...] = jnp.where(live, 0.0, -jnp.inf)
    for c in slab_copies:
        c.wait()
    local[12].wait()

    def wait_q(k, carry):
        for c in q_copies(k):
            c.wait_recv()
        return carry

    lax.fori_loop(1, n, wait_q, 0, unroll=unroll)
    qn = qn_all[...].astype(f32).reshape(rows, qn_all.shape[2]).astype(bf16)
    qr = qr_all[...].astype(f32).reshape(rows, qr_all.shape[2]).astype(bf16)
    qn_head = dot(sel_head, qn)
    for h in range(HEADS):
        at = slice(h * slots, (h + 1) * slots)
        full = dot(qn_head[at].astype(bf16), uk0[h])
        for t in range(qlat.shape[0]):
            qlat[t, at, :] = full[:, t * lanes:(t + 1) * lanes]
    r_slot = dot(sel_hot, qr).astype(bf16)

    for j in range(slots):
        at = slice(j * HEADS, (j + 1) * HEADS)
        q_slot = jnp.concatenate(
            [qlat[t, pl.ds(j, HEADS, stride=slots), :] for t in range(qlat.shape[0])], axis=1
        ).astype(bf16)
        score[at, :] = dot(q_slot, keys[j, :LATENT]) + dot(r_slot[at], keys[j, LATENT:])
    masked = score[...] * score_scale + dead[...]
    slot_max = jnp.max(masked, axis=1, keepdims=True)
    stat_max = jnp.max(jnp.where(sel, slot_max, neg_fill), axis=0, keepdims=True)
    group_max = jnp.max(jnp.where(sel, stat_max, neg_fill), axis=1, keepdims=True)
    weight = jnp.exp(masked - group_max).astype(bf16)
    slot_sum = jnp.sum(weight.astype(f32), axis=1, keepdims=True)
    stat_sum = row_sum(sel, jnp.broadcast_to(slot_sum, sel.shape))
    parts = [
        dot_t(weight[j * HEADS:(j + 1) * HEADS], keys[j, :LATENT]).astype(bf16)
        for j in range(slots)
    ]

    dense = dot(back, jnp.concatenate(parts, axis=0))
    for h in range(HEADS):
        part = dot(dense[h * batch:(h + 1) * batch].astype(bf16), uv0[h])
        proj[pl.ds(h, batch, stride=HEADS), :] = part
    outbox[...] = proj[...].reshape(outbox.shape).astype(bf16)
    stats[me] = jnp.concatenate([stat_max, stat_sum], axis=0)
    inbox[me] = outbox[me]

    def o_copies(k):
        return (
            remote(outbox.at[lax.rem(me + k, n)], inbox.at[me], o_send, o_recv, k),
            remote(stats.at[me], stats.at[me], st_send, st_recv, k),
        )

    def send_o(k, carry):
        for c in o_copies(k):
            c.start()
        return carry

    spread(send_o)

    qn0 = widen(qn_all[me].astype(f32)).astype(bf16)
    qr0 = widen(qr_all[me].astype(f32)).astype(bf16)
    ql0 = per_head(qn0, lambda i: uk0[head0 + i]).astype(bf16)
    own_score = own_scores(ql0, qr0, new0)
    new_in = jnp.broadcast_to(new0[:, :LATENT], (pad, LATENT)).astype(bf16)
    new_out = per_head(new_in, lambda i: uv0[head0 + i])

    def wait_sent(k, carry):
        for c in q_copies(k):
            c.wait_send()
        return carry

    lax.fori_loop(1, n, wait_sent, 0, unroll=unroll)

    def wait_o(k, carry):
        for c in o_copies(k):
            c.wait_recv()
        return carry

    lax.fori_loop(1, n, wait_o, 0, unroll=unroll)
    got_max = stats[:, 0, :]
    got_sum = stats[:, 1, :]
    far_max = jnp.max(got_max, axis=0, keepdims=True)
    got_f = jnp.exp(got_max - far_max)
    far_sum = jnp.sum(got_sum * got_f, axis=0, keepdims=True)
    mine = iota((rows_dev, rows), 1) == start + iota((rows_dev, rows), 0)

    def own_rows(x):
        return lane_sum(mine, jnp.broadcast_to(x, mine.shape))

    acc = jnp.zeros((rows_dev, proj.shape[1]), f32)
    for s in range(n):
        acc = acc + own_rows(got_f[s:s + 1]) * inbox[s].astype(f32)
    far_max = own_rows(far_max)
    far_sum = own_rows(far_sum)
    own_score = own_score[:rows_dev]
    top = jnp.maximum(own_score, far_max)
    own_f = jnp.exp(own_score - top)
    far_f = jnp.exp(far_max - top)
    total = own_f + far_sum * far_f
    out[0] = ((own_f * new_out[:rows_dev] + acc * far_f) / total).astype(bf16)

    def wait_o_sent(k, carry):
        for c in o_copies(k):
            c.wait_send()
        return carry

    lax.fori_loop(1, n, wait_o_sent, 0, unroll=unroll)


def shards(
    q_nope, q_rope, w_uk, w_uv, new_latent, shallow_cache, slot_positions, slab_map,
    deep_cache, deep_positions, lengths,
):
    n = lax.axis_size("holders")
    rows_dev, nope = q_nope.shape[1:]
    rope = q_rope.shape[2]
    slots, slab, width = shallow_cache.shape[1:]
    batch = new_latent.shape[1]
    value = w_uv.shape[3]
    deep_tok = deep_cache.shape[2]
    dma = pltpu.SemaphoreType.DMA
    any_spec = pl.BlockSpec(memory_space=pl.ANY)
    return pl.pallas_call(
        functools.partial(kernel, n, (rows_dev, slots, batch)),
        out_shape=jax.ShapeDtypeStruct((q_nope.shape[0], rows_dev, value), bf16),
        in_specs=[pl.BlockSpec(memory_space=pltpu.SMEM)] + [any_spec] * 10,
        out_specs=pl.BlockSpec(memory_space=pltpu.VMEM),
        scratch_shapes=[
            pltpu.VMEM((n, rows_dev, nope), bf16),
            pltpu.VMEM((n, rows_dev, rope), bf16),
            pltpu.VMEM((rows_dev, nope), bf16),
            pltpu.VMEM((rows_dev, rope), bf16),
            pltpu.VMEM(w_uk.shape[1:], bf16),
            pltpu.VMEM(w_uv.shape[1:], bf16),
            pltpu.VMEM((rows_dev,) + w_uk.shape[2:], bf16),
            pltpu.VMEM((rows_dev,) + w_uv.shape[2:], bf16),
            pltpu.VMEM(new_latent.shape, bf16),
            pltpu.VMEM((slots, width, slab), bf16),
            pltpu.VMEM((slots, slab), jnp.int32),
            pltpu.VMEM(slab_map.shape, jnp.int32),
            pltpu.VMEM((width, deep_tok), bf16),
            pltpu.VMEM((batch, deep_tok), jnp.int32),
            pltpu.VMEM((LATENT // 128, slots * HEADS, 128), f32),
            pltpu.VMEM((slots * HEADS, slab), f32),
            pltpu.VMEM((slots * HEADS, slab), f32),
            pltpu.VMEM((n * rows_dev, value), f32),
            pltpu.VMEM((n, rows_dev, value), bf16),
            pltpu.VMEM((n, rows_dev, value), bf16),
            pltpu.VMEM((n, 2, n * rows_dev), f32),
            dma((13,)),
            dma((slots,)),
            dma((n,)),
            dma((n,)),
            dma((n,)),
            dma((n,)),
            dma((n,)),
            dma((n,)),
            dma((n,)),
            dma((n,)),
        ],
        compiler_params=pltpu.CompilerParams(
            collective_id=0, has_side_effects=True, vmem_limit_bytes=60 * 1024 * 1024
        ),
    )(
        lengths, q_nope, q_rope, w_uk, w_uv, new_latent, jnp.swapaxes(shallow_cache, 2, 3),
        slot_positions, slab_map, jnp.swapaxes(deep_cache, 2, 3), deep_positions,
    )


def solution(mesh):
    return jax.shard_map(
        shards,
        mesh=mesh,
        in_specs=(
            P(None, ("groups", "holders"), None),
            P(None, ("groups", "holders"), None),
            P(),
            P(),
            P(None, "groups", None),
            P(None, ("groups", "holders"), None, None),
            P(None, ("groups", "holders"), None),
            P(None, "groups"),
            P(None, "groups", None, None),
            P(None, "groups", None),
            P("groups"),
        ),
        out_specs=P(None, ("groups", "holders"), None),
        check_vma=False,
    )
```
